32 devices in a mesh: section: 4 (over x, core), obs: 8 (over z, y).
Axes of the slice: x: 2, y: 2, z: 4, core: 2. Of those that a mesh axis runs over, the one named last changes fastest.
Arguments:
- predictors: bfloat16 [4, 4, 20, 32768], P('section', None, None, 'obs'), may hold values from -5 to 5
- departures: float32 [4, 4, 32768], P('section', None, 'obs'), may hold values from -30 to 30
- obs_precision: float32 [4, 4, 32768], P('section', None, 'obs'), may hold values from 0.3 to 3
- qc_pass: int32 [4, 4, 32768], P('section', None, 'obs'), may hold values 0 or 1
- block_channel: int32 [4, 4, 256], P('section', None, 'obs'), may hold values from 0 to 2047, as said below
- stream_order: int32 [4], replicated, may hold values from 0 to 3, each once
- prior_coeffs: float32 [4, 20, 2048], P(None, None, 'obs'), may hold values from -1 to 1
- prior_info: float32 [4, 210, 2048], P(None, None, 'obs'), may hold values from -1 to 32, as said below
- memory_factor: float32 [2048], P('obs'), may hold values from 0.5 to 0.98
Outputs:
- coeffs: float32 [4, 4, 20, 2048], P('section', None, None, 'obs')
- information: float32 [4, 4, 210, 2048], P('section', None, None, 'obs')
The draws below stay inside these ranges and needn't reach their ends.
Inputs may be any that keep to these rules, and one draw needn't show every extreme that they name: `block_channel`: among the 32 row blocks of one index of obs, at most 8 have channels in any one range of the 256 channels from a multiple of 256; in every window and stream one such range holds exactly 8 blocks of every index of obs. `stream_order`: each stream appears once. `prior_info`: for every stream and channel the 210 entries are the upper triangle, row by row, of a symmetric positive definite matrix of order 20.
All inputs are finite; a program needn't handle non-finite values. No bound on the sum of `qc_pass` on one device may be relied on, other than what follows from the above.
Results may differ from the reference program's by a relative error of at most 0.0038.
Values sent between devices are 32-bit elements; how exact they have to be, the bound alone decides.
No kernel may reach another device: no remote copies, remote signals or barrier semaphores. Data moves between devices by JAX's collectives and lax.ppermute only.
A program may use at most 64 MiB of HBM per device.

```python
import math
import jax
import jax.numpy as jnp
import numpy as np
from jax import lax

NPRED = 20
CH = 2048
BLOCK_ROWS = 128
STREAMS = 4
WINDOWS = 4
ROWS = 32768
NB_DEV = 32
NBLK = 256
CH_DEV = 256
CAP = 8


def observation_fields(base_key):
    pred_key, truth_key, noise_key = jax.random.split(jax.random.fold_in(base_key, 11), 3)
    values = jax.random.truncated_normal(pred_key, -5.0, 5.0, (WINDOWS, STREAMS, NPRED, ROWS), jnp.float32)
    true_coeffs = 0.25 * jax.random.truncated_normal(truth_key, -4.0, 4.0, (WINDOWS, STREAMS, NPRED, NBLK), jnp.float32)
    signal = jnp.einsum('wspbr,wspb->wsbr', values.reshape(WINDOWS, STREAMS, NPRED, NBLK, BLOCK_ROWS), true_coeffs).reshape(WINDOWS, STREAMS, ROWS)
    position = jnp.arange(ROWS, dtype=jnp.float32) / ROWS
    spread = 1.0 + 2.0 * position
    noise_draw = jax.random.truncated_normal(noise_key, -5.0, 5.0, (WINDOWS, STREAMS, ROWS), jnp.float32)
    return (values, jnp.clip(signal + spread * noise_draw, -30.0, 30.0))


def draw_predictors(key, part):
    return observation_fields(key)[0].astype(jnp.bfloat16)


def draw_departures(key, part):
    return observation_fields(key)[1]


def draw_block_channel(key, part):
    owner_count = NBLK // NB_DEV

    def one_group(group_key):
        pick_key, device_key = jax.random.split(group_key)
        special = jax.random.randint(pick_key, (), 0, owner_count)

        def one_device(own_key):
            list_key, shuffle_key, inner_key = jax.random.split(own_key, 3)
            others = jax.random.permutation(list_key, (owner_count - 1) * CAP)[:NB_DEV - CAP]
            other_owner = (others // CAP + special + 1) % owner_count
            owners = jnp.concatenate([jnp.full((CAP,), special, jnp.int32), other_owner.astype(jnp.int32)])
            owners = jax.random.permutation(shuffle_key, owners)
            inner_channel = jax.random.randint(inner_key, (NB_DEV,), 0, CH_DEV)
            return (owners * CH_DEV + inner_channel).astype(jnp.int32)
        return jax.vmap(one_device)(jax.random.split(device_key, owner_count)).reshape(NBLK)
    groups = jax.vmap(one_group)(jax.random.split(jax.random.fold_in(key, 31), WINDOWS * STREAMS))
    return groups.reshape(WINDOWS, STREAMS, NBLK)


def draw_prior_info(key, part):
    raw_key, margin_key = jax.random.split(jax.random.fold_in(key, 23))
    raw = jax.random.uniform(raw_key, (STREAMS, CH, NPRED, NPRED), jnp.float32, -1.0, 1.0)
    identity = jnp.eye(NPRED, dtype=jnp.float32)
    coupling = 0.5 * (raw + jnp.swapaxes(raw, 2, 3)) * (1.0 - identity)
    margin = jnp.exp(jax.random.uniform(margin_key, (STREAMS, CH, NPRED), jnp.float32, math.log(2.0), math.log(12.0)))
    leading = jnp.sum(jnp.abs(coupling), axis=3) + margin
    matrix = coupling + leading[..., None] * identity
    upper_index = np.array([i * NPRED + j for i in range(NPRED) for j in range(i, NPRED)], dtype=np.int32)
    packed = matrix.reshape(STREAMS, CH, NPRED * NPRED)[:, :, upper_index]
    return jnp.swapaxes(packed, 1, 2)


def place_ends(drawn, key, smallest, top_value):
    longest = drawn.shape.index(max(drawn.shape))
    spots = []
    for shift in (0, 1):
        where = [jax.random.randint(jax.random.fold_in(key, axis), (), 0, length) for axis, length in enumerate(drawn.shape)]
        where[longest] = (where[longest] + shift) % drawn.shape[longest]
        spots.append(tuple(where))
    return drawn.at[spots[0]].set(smallest).at[spots[1]].set(top_value)


def levels(stream_key, dims, pieces, least, top_value):
    factor_of = 1.0
    for axis_at, parts in pieces:
        heights = jax.random.uniform(jax.random.fold_in(jax.random.fold_in(stream_key, 6), axis_at), (parts,), jnp.float32, least / len(pieces), top_value / len(pieces))
        factor_of = factor_of * jnp.repeat(jnp.exp(heights), dims[axis_at] // parts).reshape((-1,) + (1,) * (len(dims) - 1 - axis_at))
    return factor_of


def scatter_about(key, extent, scale, reach, cuts=(), held_as=jnp.bfloat16):
    drawn = scale * jax.random.normal(key, extent, jnp.float32)
    if cuts:
        drawn = drawn * levels(key, extent, cuts, -0.22, 0.18)
    return jnp.clip(drawn, -reach, reach).astype(held_as)


def setup_inputs(seed: int = 0) -> dict:
    splits = jax.random.split(jax.random.key(seed), 10)
    predictors = draw_predictors(jax.random.fold_in(splits[9], 71), 0)
    departures = draw_departures(jax.random.fold_in(splits[9], 71), 0)
    obs_precision = jnp.clip(jnp.exp(math.log(3.0) - 2.3025851 * jax.random.uniform(splits[2], (WINDOWS, STREAMS, ROWS), jnp.float32) ** levels(splits[2], (WINDOWS, STREAMS, ROWS), ((0, 4), (2, 8)), -0.2, 0.2)), 0.3, 3.0)
    qc_pass = place_ends((jax.random.randint(splits[3], (WINDOWS, STREAMS, ROWS), 0, 4) < 3).astype(jnp.int32), jax.random.fold_in(splits[3], 1), 0, 1)
    block_channel = draw_block_channel(jax.random.fold_in(splits[9], 71), 0)
    stream_order = jax.random.permutation(splits[5], STREAMS).astype(jnp.int32)
    prior_coeffs = scatter_about(splits[6], (STREAMS, NPRED, CH), 0.25, 1.0, ((2, 8),), jnp.float32)
    prior_info = draw_prior_info(jax.random.fold_in(splits[9], 71), 0)
    memory_factor = jnp.clip(jnp.exp(math.log(0.98) - 0.6729445 * jax.random.uniform(splits[8], (CH,), jnp.float32) ** levels(splits[8], (CH,), ((0, 8),), -0.2, 0.2)), 0.5, 0.98)
    return {"predictors": predictors, "departures": departures, "obs_precision": obs_precision, "qc_pass": qc_pass, "block_channel": block_channel, "stream_order": stream_order, "prior_coeffs": prior_coeffs, "prior_info": prior_info, "memory_factor": memory_factor}


HUBER_SQ = 9.0
PRIOR_WEIGHT = 64.0

def upper_positions(dimension):
    return np.array([i * dimension + j for i in range(dimension) for j in range(i, dimension)], dtype=np.int32)

def solve_packed(packed, target):
    dimension = target.shape[0]
    placing = {}
    counter = 0
    for i in range(dimension):
        for j in range(i, dimension):
            placing[i, j] = counter
            counter += 1
    factor = [[None] * dimension for i in range(dimension)]
    for j in range(dimension):
        pivot_root = jnp.sqrt(packed[placing[j, j]] - sum((factor[j][k] * factor[j][k] for k in range(j))))
        factor[j][j] = pivot_root
        for i in range(j + 1, dimension):
            factor[i][j] = (packed[placing[j, i]] - sum((factor[i][k] * factor[j][k] for k in range(j)))) / pivot_root
    forward = []
    for i in range(dimension):
        forward.append((target[i] - sum((factor[i][k] * forward[k] for k in range(i)))) / factor[i][i])
    backward = [None] * dimension
    for i in reversed(range(dimension)):
        backward[i] = (forward[i] - sum((factor[k][i] * backward[k] for k in range(i + 1, dimension)))) / factor[i][i]
    return jnp.stack(backward)

def stream_update(beta_prior, info_prior, predicted, departed, precision, passed, channel):
    pred_count = predicted.shape[0]
    block_count = channel.shape[0]
    block_width = departed.shape[0] // block_count
    shaped = predicted.astype(jnp.float32).reshape(pred_count, block_count, block_width)
    block_coeffs = jnp.take(beta_prior, channel, axis=1)
    offset = lax.optimization_barrier(jnp.sum(shaped * block_coeffs[:, :, None], axis=0))
    residual = departed.reshape(block_count, block_width) - offset
    scale_row = precision.reshape(block_count, block_width)
    weight = passed.reshape(block_count, block_width).astype(jnp.float32) * scale_row / (1.0 + scale_row * residual * residual / HUBER_SQ)
    weighted = lax.optimization_barrier((weight[None] * shaped).astype(jnp.bfloat16)).astype(jnp.float32)
    chi_square = jnp.sum(weight * residual * residual)
    passed_count = jnp.sum(passed.astype(jnp.float32))
    inflation = (chi_square + PRIOR_WEIGHT) / (passed_count + PRIOR_WEIGHT)
    gram_upper = jnp.einsum('ibr,jbr->bij', weighted, shaped).reshape(block_count, pred_count * pred_count)[:, upper_positions(pred_count)]
    gradient = jnp.einsum('ibr,br->bi', weighted, residual)
    block_sums = jnp.concatenate([gram_upper, gradient], axis=1)
    normal = jax.ops.segment_sum(block_sums, channel, num_segments=CH).T
    tri_count = gram_upper.shape[1]
    info_post = info_prior + normal[:tri_count] / inflation
    beta_post = beta_prior + solve_packed(info_post, normal[tri_count:] / inflation)
    return (beta_post, info_post)

def reference(predictors, departures, obs_precision, qc_pass, block_channel, stream_order, prior_coeffs, prior_info, memory_factor):

    def window_step(state_pair, window):
        beta_prior, info_prior = state_pair

        def select_window(source):
            return jnp.take(lax.dynamic_index_in_dim(source, window, 0, keepdims=False), stream_order, axis=0)
        beta_post, info_post = jax.vmap(stream_update)(beta_prior, info_prior, select_window(predictors), select_window(departures), select_window(obs_precision), select_window(qc_pass), select_window(block_channel))
        return ((beta_post, memory_factor[None, None, :] * info_post), (beta_post, info_post))
    initial = (jnp.take(prior_coeffs, stream_order, axis=0), jnp.take(prior_info, stream_order, axis=0))
    final_state, outputs = lax.scan(window_step, initial, jnp.arange(WINDOWS, dtype=jnp.int32))
    return (outputs[0], outputs[1])
```

```python
import jax
import jax.numpy as jnp
import numpy as np
from jax import lax
from jax.sharding import PartitionSpec as P

HUBER_SQ = 9.0
PRIOR_WEIGHT = 64.0


def upper_positions(dimension):
    return np.array(
        [i * dimension + j for i in range(dimension) for j in range(i, dimension)], dtype=np.int32
    )


def solve_packed(packed, target):
    dimension = target.shape[0]
    placing = {}
    counter = 0
    for i in range(dimension):
        for j in range(i, dimension):
            placing[i, j] = counter
            counter += 1
    factor = [[None] * dimension for i in range(dimension)]
    for j in range(dimension):
        pivot_root = jnp.sqrt(
            packed[placing[j, j]] - sum((factor[j][k] * factor[j][k] for k in range(j)))
        )
        factor[j][j] = pivot_root
        for i in range(j + 1, dimension):
            factor[i][j] = (
                packed[placing[j, i]] - sum((factor[i][k] * factor[j][k] for k in range(j)))
            ) / pivot_root
    forward = []
    for i in range(dimension):
        forward.append(
            (target[i] - sum((factor[i][k] * forward[k] for k in range(i)))) / factor[i][i]
        )
    backward = [None] * dimension
    for i in reversed(range(dimension)):
        backward[i] = (
            forward[i] - sum((factor[k][i] * backward[k] for k in range(i + 1, dimension)))
        ) / factor[i][i]
    return jnp.stack(backward)


def block_rows(fields, block_coeffs, pred_count):
    block_count = block_coeffs.shape[1]
    row_count = fields.shape[1]
    block_width = row_count // block_count
    upper_index = upper_positions(pred_count)
    shaped = fields[:pred_count].reshape(pred_count, block_count, block_width)
    departed = fields[pred_count].reshape(block_count, block_width)
    scale_row = fields[pred_count + 1].reshape(block_count, block_width)
    offset = jnp.sum(shaped * block_coeffs[:, :, None], axis=0)
    residual = departed - offset
    weight = scale_row / (1.0 + scale_row * residual * residual / HUBER_SQ)
    weighted = lax.reduce_precision(weight[None] * shaped, 8, 7)
    chi_square = jnp.sum(weight * residual * residual)
    passed_count = jnp.sum((scale_row > 0.0).astype(jnp.float32))
    gram_full = lax.dot_general(
        weighted, shaped, (((2,), (2,)), ((1,), (1,))), preferred_element_type=jnp.float32
    )
    gram_upper = gram_full.reshape(block_count, pred_count * pred_count)[:, upper_index]
    gradient = jnp.sum(weighted * residual[None], axis=2).T
    return (jnp.concatenate([gram_upper, gradient], axis=1), jnp.stack([chi_square, passed_count]))


def local(
    predictors,
    departures,
    obs_precision,
    qc_pass,
    block_channel,
    stream_order,
    prior_coeffs,
    prior_info,
    memory_factor,
):
    sections = lax.axis_size("section")
    owners = lax.axis_size("obs")
    section_place = lax.axis_index("section")
    stream_count = stream_order.shape[0]
    local_channels = memory_factor.shape[0]
    block_count = block_channel.shape[2]
    pred_count = prior_coeffs.shape[1]
    tri_count = prior_info.shape[1]
    column_count = tri_count + pred_count
    capacity = 2 * block_count // owners
    slots = owners * capacity
    highest = lax.Precision.HIGHEST
    groups = -(-stream_count // sections)

    def turn(array, axis):
        return lax.all_to_all(array, axis, split_axis=0, concat_axis=0, tiled=True)

    def select_rows(hot, values, dims):
        return lax.dot_general(
            hot, values, (dims, ((), ())), precision=highest, preferred_element_type=jnp.float32
        )

    coeff_parts = []
    info_parts = []
    for group in range(groups):
        wanted = np.minimum(np.arange(sections) + group * sections, stream_count - 1)
        streams = stream_order[wanted]
        own_stream = stream_order[jnp.minimum(section_place + group * sections, stream_count - 1)]
        kept = jnp.take(obs_precision[0] * qc_pass[0].astype(jnp.float32), streams, axis=0)
        fields = jnp.concatenate(
            [
                jnp.take(predictors[0], streams, axis=0).astype(jnp.float32),
                jnp.take(departures[0], streams, axis=0)[:, None],
                kept[:, None],
            ],
            axis=1,
        )
        channel = turn(jnp.take(block_channel[0], streams, axis=0), "section")
        fields = turn(fields, "section")
        owner_index = channel // local_channels
        owner_hot = (owner_index[:, :, None] == jnp.arange(owners)).astype(jnp.int32)
        ranking = jnp.sum((jnp.cumsum(owner_hot, axis=1) - 1) * owner_hot, axis=2)
        slot_of = owner_index * capacity + ranking
        is_slot = slot_of[:, :, None] == jnp.arange(slots, dtype=jnp.int32)
        placing = is_slot.astype(jnp.float32)
        asked = jnp.sum(jnp.where(is_slot, (channel % local_channels)[:, :, None] + 1, 0), axis=1) - 1
        asked = asked.reshape(sections, owners, capacity).swapaxes(0, 1)
        asked = turn(asked, "obs").swapaxes(0, 1).reshape(sections, slots)
        asked_hot = (asked[:, :, None] == jnp.arange(local_channels)).astype(jnp.float32)

        beta = lax.dynamic_index_in_dim(prior_coeffs, own_stream, 0, keepdims=False)
        kept_info = lax.dynamic_index_in_dim(prior_info, own_stream, 0, keepdims=False)
        results = []
        for w in range(sections):
            sent = select_rows(asked_hot[w], beta, ((1,), (1,)))
            got = turn(sent.reshape(owners, capacity, pred_count), "obs")
            block_coeffs = select_rows(got.reshape(slots, pred_count), placing[w], ((0,), (1,)))
            block_sums, statistics = block_rows(fields[w], block_coeffs, pred_count)
            rows = select_rows(placing[w], block_sums, ((0,), (0,)))
            rows = jnp.concatenate(
                [rows, jnp.broadcast_to(statistics[None], (slots, 2))], axis=1
            ).reshape(owners, capacity, column_count + 2)
            rows = turn(rows, "obs")
            totals = jnp.sum(rows[:, 0, column_count:], axis=0)
            inflation = (totals[0] + PRIOR_WEIGHT) / (totals[1] + PRIOR_WEIGHT)
            normal = (
                select_rows(
                    rows.reshape(slots, column_count + 2)[:, :column_count],
                    asked_hot[w],
                    ((0,), (0,)),
                )
                / inflation
            )
            info_post = kept_info + normal[:tri_count]
            beta = beta + solve_packed(info_post, normal[tri_count:])
            kept_info = memory_factor[None] * info_post
            results.append(jnp.concatenate([beta, info_post], axis=0))
        landed = turn(jnp.stack(results), "section")
        count = min(sections, stream_count - group * sections)
        coeff_parts.append(landed[:count, :pred_count])
        info_parts.append(landed[:count, pred_count:])
    if groups == 1:
        return (coeff_parts[0][None], info_parts[0][None])
    return (jnp.concatenate(coeff_parts)[None], jnp.concatenate(info_parts)[None])


def solution(mesh):
    in_specs = (
        P("section", None, None, "obs"),
        P("section", None, "obs"),
        P("section", None, "obs"),
        P("section", None, "obs"),
        P("section", None, "obs"),
        P(),
        P(None, None, "obs"),
        P(None, None, "obs"),
        P("obs"),
    )
    out_specs = (P("section", None, None, "obs"), P("section", None, None, "obs"))
    return jax.shard_map(local, mesh=mesh, in_specs=in_specs, out_specs=out_specs, check_vma=False)
```

```python
import jax
import jax.numpy as jnp
import numpy as np
from jax import lax
from jax.experimental import pallas as pl
from jax.experimental.pallas import tpu as pltpu
from jax.sharding import PartitionSpec as P

HUBER_SQ = 9.0
PRIOR_WEIGHT = 64.0


def upper_positions(dimension):
    return np.array(
        [i * dimension + j for i in range(dimension) for j in range(i, dimension)], dtype=np.int32
    )


def update_kernel(normal_ref, kept_ref, beta_ref, inflation_ref, result_ref, factor_ref, work_ref):
    dimension = beta_ref.shape[0]
    tri_count = kept_ref.shape[0]
    padded, channels = work_ref.shape
    inverse = 1.0 / inflation_ref[0, 0]
    info = kept_ref[...] + normal_ref[pl.ds(0, tri_count), :] * inverse
    result_ref[pl.ds(dimension, tri_count), :] = info
    work_ref[pl.ds(0, dimension), :] = normal_ref[pl.ds(tri_count, dimension), :] * inverse
    start = 0
    for j in range(dimension):
        length = dimension - j
        factor_ref[j, pl.ds(j, length), :] = result_ref[pl.ds(dimension + start, length), :]
        start += length
    roots = []
    forward = []
    for j in range(dimension):
        low = 8 * (j // 8)
        high = padded - low
        column = factor_ref[j, pl.ds(low, high), :]
        for k in range(j):
            column = column - factor_ref[k, pl.ds(low, high), :] * factor_ref[k, pl.ds(j, 1), :]
        inverse_root = 1.0 / jnp.sqrt(column[j - low : j - low + 1, :])
        column = column * inverse_root
        factor_ref[j, pl.ds(low, high), :] = column
        target = work_ref[pl.ds(low, high), :]
        solved = target[j - low : j - low + 1, :] * inverse_root
        work_ref[pl.ds(low, high), :] = target - column * solved
        roots.append(inverse_root)
        forward.append(solved)
    line = lax.broadcasted_iota(jnp.int32, (padded, channels), 0)
    answer = jnp.zeros((padded, channels), jnp.float32)
    for i in reversed(range(dimension)):
        low = 8 * (i // 8)
        high = padded - low
        places = line[low:, :]
        below = jnp.logical_and(places > i, places < dimension)
        terms = jnp.where(below, factor_ref[i, pl.ds(low, high), :] * answer[low:, :], 0.0)
        value = (forward[i] - jnp.sum(terms, axis=0, keepdims=True)) * roots[i]
        answer = jnp.where(line == i, value, answer)
    result_ref[pl.ds(0, dimension), :] = beta_ref[...] + answer[:dimension, :]


def update_state(normal, kept_info, beta, inflation):
    dimension, channels = beta.shape
    padded = -(-dimension // 8) * 8
    whole = pl.BlockSpec(memory_space=pltpu.VMEM)
    return pl.pallas_call(
        update_kernel,
        out_shape=jax.ShapeDtypeStruct(normal.shape, jnp.float32),
        in_specs=[whole, whole, whole, pl.BlockSpec(memory_space=pltpu.SMEM)],
        out_specs=whole,
        scratch_shapes=[
            pltpu.VMEM((dimension, padded, channels), jnp.float32),
            pltpu.VMEM((padded, channels), jnp.float32),
        ],
        name="update_state",
    )(normal, kept_info, beta, inflation.reshape(1, 1))


def block_rows(fields, block_coeffs, pred_count):
    block_count = block_coeffs.shape[1]
    row_count = fields.shape[1]
    block_width = row_count // block_count
    upper_index = upper_positions(pred_count)
    shaped = fields[:pred_count].reshape(pred_count, block_count, block_width)
    departed = fields[pred_count].reshape(block_count, block_width)
    scale_row = fields[pred_count + 1].reshape(block_count, block_width)
    offset = jnp.sum(shaped * block_coeffs[:, :, None], axis=0)
    residual = departed - offset
    weight = scale_row / (1.0 + scale_row * residual * residual / HUBER_SQ)
    weighted = lax.reduce_precision(weight[None] * shaped, 8, 7)
    chi_square = jnp.sum(weight * residual * residual)
    passed_count = jnp.sum((scale_row > 0.0).astype(jnp.float32))
    gram_full = lax.dot_general(
        weighted, shaped, (((2,), (2,)), ((1,), (1,))), preferred_element_type=jnp.float32
    )
    gram_upper = gram_full.reshape(block_count, pred_count * pred_count)[:, upper_index]
    gradient = jnp.sum(weighted * residual[None], axis=2).T
    return (jnp.concatenate([gram_upper, gradient], axis=1), jnp.stack([chi_square, passed_count]))


def local(
    predictors,
    departures,
    obs_precision,
    qc_pass,
    block_channel,
    stream_order,
    prior_coeffs,
    prior_info,
    memory_factor,
):
    sections = lax.axis_size("section")
    owners = lax.axis_size("obs")
    section_place = lax.axis_index("section")
    stream_count = stream_order.shape[0]
    local_channels = memory_factor.shape[0]
    block_count = block_channel.shape[2]
    pred_count = prior_coeffs.shape[1]
    tri_count = prior_info.shape[1]
    column_count = tri_count + pred_count
    capacity = 2 * block_count // owners
    slots = owners * capacity
    highest = lax.Precision.HIGHEST
    groups = -(-stream_count // sections)

    def turn(array, axis):
        return lax.all_to_all(array, axis, split_axis=0, concat_axis=0, tiled=True)

    def select_rows(hot, values, dims):
        return lax.dot_general(
            hot, values, (dims, ((), ())), precision=highest, preferred_element_type=jnp.float32
        )

    coeff_parts = []
    info_parts = []
    for group in range(groups):
        wanted = np.minimum(np.arange(sections) + group * sections, stream_count - 1)
        streams = stream_order[wanted]
        own_stream = stream_order[jnp.minimum(section_place + group * sections, stream_count - 1)]
        kept = jnp.take(obs_precision[0] * qc_pass[0].astype(jnp.float32), streams, axis=0)
        fields = jnp.concatenate(
            [
                jnp.take(predictors[0], streams, axis=0).astype(jnp.float32),
                jnp.take(departures[0], streams, axis=0)[:, None],
                kept[:, None],
            ],
            axis=1,
        )
        channel = turn(jnp.take(block_channel[0], streams, axis=0), "section")
        own_fields = lax.dynamic_index_in_dim(fields, section_place, 0, keepdims=False)
        first_routes = [own_fields]
        later_routes = [own_fields]
        for r in range(1, sections):
            target = (section_place + r) % sections
            going = lax.dynamic_index_in_dim(fields, target, 0, keepdims=False)
            first_routes.append(lax.ppermute(going, "section", [(0, r)]))
            pairs = [(p, (p + r) % sections) for p in range(1, sections)]
            later_routes.append(lax.ppermute(going, "section", pairs))
        owner_index = channel // local_channels
        owner_hot = (owner_index[:, :, None] == jnp.arange(owners)).astype(jnp.int32)
        ranking = jnp.sum((jnp.cumsum(owner_hot, axis=1) - 1) * owner_hot, axis=2)
        slot_of = owner_index * capacity + ranking
        is_slot = slot_of[:, :, None] == jnp.arange(slots, dtype=jnp.int32)
        placing = is_slot.astype(jnp.float32)
        asked = jnp.sum(jnp.where(is_slot, (channel % local_channels)[:, :, None] + 1, 0), axis=1) - 1
        asked = asked.reshape(sections, owners, capacity).swapaxes(0, 1)
        asked = turn(asked, "obs").swapaxes(0, 1).reshape(sections, slots)
        asked_hot = (asked[:, :, None] == jnp.arange(local_channels)).astype(jnp.float32)

        beta = lax.dynamic_index_in_dim(prior_coeffs, own_stream, 0, keepdims=False)
        kept_info = lax.dynamic_index_in_dim(prior_info, own_stream, 0, keepdims=False)
        results = []
        for w in range(sections):
            sent = select_rows(asked_hot[w], beta, ((1,), (1,)))
            got = turn(sent.reshape(owners, capacity, pred_count), "obs")
            block_coeffs = select_rows(got.reshape(slots, pred_count), placing[w], ((0,), (1,)))
            if w == 1:
                later_routes, block_coeffs = lax.optimization_barrier((later_routes, block_coeffs))
            routes = first_routes if w == 0 else later_routes
            window_fields = lax.select_n((section_place - w) % sections, *routes)
            block_sums, statistics = block_rows(window_fields, block_coeffs, pred_count)
            rows = select_rows(placing[w], block_sums, ((0,), (0,)))
            rows = jnp.concatenate(
                [rows, jnp.broadcast_to(statistics[None], (slots, 2))], axis=1
            ).reshape(owners, capacity, column_count + 2)
            rows = turn(rows, "obs")
            totals = jnp.sum(rows[:, 0, column_count:], axis=0)
            inflation = (totals[0] + PRIOR_WEIGHT) / (totals[1] + PRIOR_WEIGHT)
            normal = select_rows(
                rows.reshape(slots, column_count + 2)[:, :column_count],
                asked_hot[w],
                ((0,), (0,)),
            )
            result = update_state(normal, kept_info, beta, inflation)
            beta = result[:pred_count]
            kept_info = memory_factor[None] * result[pred_count:]
            results.append(result)
        landed = turn(jnp.stack(results), "section")
        count = min(sections, stream_count - group * sections)
        coeff_parts.append(landed[:count, :pred_count])
        info_parts.append(landed[:count, pred_count:])
    if groups == 1:
        return (coeff_parts[0][None], info_parts[0][None])
    return (jnp.concatenate(coeff_parts)[None], jnp.concatenate(info_parts)[None])


def solution(mesh):
    in_specs = (
        P("section", None, None, "obs"),
        P("section", None, "obs"),
        P("section", None, "obs"),
        P("section", None, "obs"),
        P("section", None, "obs"),
        P(),
        P(None, None, "obs"),
        P(None, None, "obs"),
        P("obs"),
    )
    out_specs = (P("section", None, None, "obs"), P("section", None, None, "obs"))
    return jax.shard_map(local, mesh=mesh, in_specs=in_specs, out_specs=out_specs, check_vma=False)
```
